32 devices in a mesh: row: 4 (over y, x), col: 8 (over z, core).
Axes of the slice: x: 2, y: 2, z: 4, core: 2. Of those that a mesh axis runs over, the one named last changes fastest.
Arguments:
- features: bfloat16 [131072, 256], P(('row', 'col')), may hold values from -6 to 6
- send_rows: int32 [32, 32, 128], P(('row', 'col')), may hold values from 0 to 4095
- counts: int32 [32, 32], P(('row', 'col')), may hold values from 112 to 128, as said below
- tile_dst: int32 [32, 64], P(('row', 'col')), may hold values from 0 to 31
- tile_src: int32 [32, 64], P(('row', 'col')), may hold values from 0 to 63, each once within a row
- tiles: int32 [32, 64, 128, 128], P(('row', 'col')), may hold values 0 or 1
- w_self: bfloat16 [256, 256], replicated, may hold values from -0.375 to 0.375
- w_neigh: bfloat16 [256, 256], replicated, may hold values from -1.5 to 1.5
- bias: float32 [256], replicated, may hold values from -1 to 1
- cotangent: bfloat16 [131072, 256], P(('row', 'col')), may hold values from -6 to 6
Outputs:
- layer_out: bfloat16 [131072, 256], P(('row', 'col'))
- grad_features: float32 [131072, 256], P(('row', 'col'))
- grad_self: float32 [256, 256], replicated
- grad_neigh: float32 [256, 256], replicated
- grad_bias: float32 [256], replicated
The draws below stay inside these ranges and needn't reach their ends.
Inputs may be any that keep to these rules, and one draw needn't show every extreme that they name: Every partition p has some q with counts[p, q] = 128.
All inputs are finite; a program needn't handle non-finite values. No bound on the sum of `tiles` on one device may be relied on, other than what follows from the above.
Results may differ from the reference program's by a relative error of at most 0.0051.
Values may be sent and summed in bfloat16 or wider, within the bound.
No kernel may reach another device: no remote copies, remote signals or barrier semaphores. Data moves between devices by JAX's collectives and lax.ppermute only.
A program may use at most 192 MiB of HBM per device.

```python
import jax
import jax.numpy as jnp
from jax import lax

F = 256
H = 256
TB = 128
R = 4096
RB = 32
SB = 64
NT = 64
NODES = 131072
DEVICES = 32


def draw_counts(key, part):
    base = jax.random.randint(jax.random.fold_in(key, 11), (DEVICES, DEVICES), 7 * TB // 8, TB + 1)
    senders = jnp.arange(DEVICES, dtype=jnp.int32)[:, None]
    readers = jnp.arange(DEVICES, dtype=jnp.int32)[None, :]
    return jnp.where(readers == (senders + 1) % DEVICES, TB, base).astype(jnp.int32)


def touch_ends(result, stream_key, smallest, top_value):
    spot = [jax.random.randint(jax.random.fold_in(stream_key, axis), (), 0, length) for axis, length in enumerate(result.shape)]
    widest = result.shape.index(max(result.shape))
    next_to = spot[:widest] + [(spot[widest] + 1) % result.shape[widest]] + spot[widest + 1:]
    return result.at[tuple(spot)].set(smallest).at[tuple(next_to)].set(top_value)


def levels(key, extent, shards, smallest, largest):
    gain, own = 1.0, jax.random.fold_in(key, 6)
    for axis_at, parts in shards:
        heights = jnp.exp(jax.random.uniform(jax.random.fold_in(own, axis_at), (parts,), jnp.float32, smallest / len(shards), largest / len(shards)))
        gain = gain * jnp.repeat(heights, extent[axis_at] // parts).reshape([-1 if axis == axis_at else 1 for axis in range(len(extent))])
    return gain


def normal_values(key, shape, deviation, limit, shards=(), kind=jnp.bfloat16):
    values = deviation * jax.random.normal(key, shape, jnp.float32)
    if shards:
        values = values * levels(key, shape, shards, -0.22, 0.18)
    return jnp.clip(values, -limit, limit).astype(kind)


def setup_inputs(seed: int = 0) -> dict:
    keys = jax.random.split(jax.random.key(seed), 11)
    return {
        "features": normal_values(keys[0], (NODES, F), 1.0, 6.0, ((0, 32),)),
        "send_rows": touch_ends(jax.random.randint(keys[1], (DEVICES, DEVICES, TB), 0, R), jax.random.fold_in(keys[1], 1), 0, R - 1).astype(jnp.int32),
        "counts": draw_counts(jax.random.fold_in(keys[10], 71), 0),
        "tile_dst": touch_ends(jax.random.randint(keys[3], (DEVICES, NT), 0, R // TB), jax.random.fold_in(keys[3], 1), 0, (R // TB) - 1).astype(jnp.int32),
        "tile_src": jax.vmap(lambda own: jax.random.permutation(own, NT))(jax.random.split(keys[4], DEVICES)).reshape((DEVICES, NT)).astype(jnp.int32),
        "tiles": touch_ends((jax.random.randint(keys[5], (DEVICES, NT, TB, TB), 0, 4) < 1).astype(jnp.int32), jax.random.fold_in(keys[5], 1), 0, 1),
        "w_self": normal_values(keys[6], (F, H), F ** -0.5, 0.375),
        "w_neigh": normal_values(keys[7], (F, H), (F // 16) ** -0.5, 1.5),
        "bias": jnp.clip(jax.random.uniform(keys[8], (H,), jnp.float32, -1.0, 1.0), -1.0, 1.0),
        "cotangent": normal_values(keys[9], (NODES, H), 1.0, 6.0, ((0, 32),)),
    }


def reference(features, send_rows, counts, tile_dst, tile_src, tiles, w_self, w_neigh, bias, cotangent):
    slots = jnp.arange(TB, dtype=jnp.int32)
    owners = jnp.arange(DEVICES, dtype=jnp.int32) * R
    inv_root = 1.0 / jnp.sqrt(jnp.float32(NODES))

    def device_step(carry, part):
        grad_all, acc_self, acc_neigh, acc_bias = carry
        start = (part * R).astype(jnp.int32)
        own = lax.dynamic_slice_in_dim(features, start, R, 0)
        cot = lax.dynamic_slice_in_dim(cotangent, start, R, 0)
        picks = lax.dynamic_index_in_dim(send_rows, part, 1, False)
        used = lax.dynamic_index_in_dim(counts, part, 1, False)
        keep = (slots[None, :] < used[:, None]).reshape(-1)
        global_rows = (picks + owners[:, None]).reshape(-1).astype(jnp.int32)
        remote = features[global_rows] * keep[:, None].astype(features.dtype)
        source = jnp.concatenate([own, remote], 0).reshape(SB, TB, F)
        dst = lax.dynamic_index_in_dim(tile_dst, part, 0, False)
        src = lax.dynamic_index_in_dim(tile_src, part, 0, False)
        adj_int = lax.dynamic_index_in_dim(tiles, part, 0, False)
        adj = adj_int.astype(jnp.float32)
        picked = source[src].astype(jnp.float32)
        prod = jnp.einsum('tij,tjf->tif', adj, picked)
        neigh = jax.ops.segment_sum(prod, dst, num_segments=RB).reshape(R, F)
        degree = jax.ops.segment_sum(lax.optimization_barrier(jnp.sum(adj_int, axis=2)).astype(jnp.float32), dst, num_segments=RB).reshape(R)
        scale = 1.0 / (1.0 + degree)
        agg = (neigh * scale[:, None]).astype(jnp.bfloat16)
        pre = jnp.dot(own, w_self, preferred_element_type=jnp.float32) + jnp.dot(agg, w_neigh, preferred_element_type=jnp.float32) + bias
        sig = jax.nn.sigmoid(pre)
        out = (pre * sig).astype(jnp.bfloat16)
        dpre = cot.astype(jnp.float32) * (sig * (1.0 + pre * (1.0 - sig)))
        dpre_b = dpre.astype(jnp.bfloat16)
        acc_self = acc_self + jnp.dot(own.T, dpre_b, preferred_element_type=jnp.float32)
        acc_neigh = acc_neigh + jnp.dot(agg.T, dpre_b, preferred_element_type=jnp.float32)
        acc_bias = acc_bias + lax.optimization_barrier(jnp.sum(dpre, axis=0))
        g_rows = (jnp.dot(dpre_b, w_neigh.T, preferred_element_type=jnp.float32) * scale[:, None]).astype(jnp.bfloat16)
        g_blocks = g_rows.reshape(RB, TB, F)[dst].astype(jnp.float32)
        back = jnp.einsum('tij,tif->tjf', adj, g_blocks)
        back_sum = jax.ops.segment_sum(back, src, num_segments=SB).reshape(SB * TB, F)
        own_grad = jnp.dot(dpre_b, w_self.T, preferred_element_type=jnp.float32) + back_sum[:R]
        back_b = back_sum[R:].astype(jnp.bfloat16)
        remote_grad = back_b.astype(jnp.float32) * keep[:, None].astype(jnp.float32)
        grad_all = grad_all.at[global_rows].add(remote_grad)
        current = lax.dynamic_slice_in_dim(grad_all, start, R, 0)
        grad_all = lax.dynamic_update_slice_in_dim(grad_all, current + own_grad, start, 0)
        return ((grad_all, acc_self, acc_neigh, acc_bias), out)
    init = (jnp.zeros((NODES, F), jnp.float32), jnp.zeros((F, H), jnp.float32), jnp.zeros((F, H), jnp.float32), jnp.zeros((H,), jnp.float32))
    final, outs = lax.scan(device_step, init, jnp.arange(DEVICES, dtype=jnp.int32))
    grad_all, acc_self, acc_neigh, acc_bias = final
    return (outs.reshape(NODES, H), grad_all, acc_self * inv_root, acc_neigh * inv_root, acc_bias * inv_root)
```

```python
import functools

import jax
import jax.numpy as jnp
from jax import lax
from jax.experimental import pallas as pl
from jax.experimental.pallas import tpu as pltpu
from jax.sharding import PartitionSpec as P

AXES = ("row", "col")
LANES = 128
VMEM = pl.BlockSpec(memory_space=pltpu.VMEM)
SMEM = pl.BlockSpec(memory_space=pltpu.SMEM)
ANY = pl.BlockSpec(memory_space=pl.ANY)
F32 = jnp.float32
BF16 = jnp.bfloat16


def matmul(a, b):
    return jnp.dot(a, b, preferred_element_type=F32)


def matmul_t(a, b):
    return lax.dot_general(a, b, (((1,), (1,)), ((), ())), preferred_element_type=F32)


def params(mib):
    return pltpu.CompilerParams(vmem_limit_bytes=mib * 1024 * 1024)


def cost(flops, nbytes):
    return pl.CostEstimate(flops=int(flops), bytes_accessed=int(nbytes), transcendentals=0)


def gather_kernel(picks_in, counts_in, x_in, out_in, picks, counts, x, out, sems, *scratch):
    rows, width = x.shape
    peers, slots = picks.shape
    halves = width // LANES
    wide, stage = scratch[:halves], scratch[halves:]
    parts = 4
    chunk = rows // parts
    step = 128
    copies = [
        pltpu.make_async_copy(picks_in, picks, sems.at[0]),
        pltpu.make_async_copy(counts_in, counts, sems.at[1]),
    ]
    for c in range(parts):
        at = pl.ds(c * chunk, chunk)
        copies.append(pltpu.make_async_copy(x_in.at[at], x.at[at], sems.at[2 + c]))
    for copy in copies:
        copy.start()
    for c in range(parts):
        copies[2 + c].wait()

        @pl.loop(c * chunk // step, (c + 1) * chunk // step)
        def _(i):
            at = pl.ds(pl.multiple_of(i * step, step), step)
            for h in range(halves):
                wide[h][at, :] = x[at, h * LANES : (h + 1) * LANES].astype(F32)

    copies[0].wait()
    copies[1].wait()

    @pl.loop(0, peers)
    def _(p):
        for k in range(slots):
            row = picks[p, k]
            for h in range(halves):
                stage[h][pl.ds(k, 1), :] = wide[h][pl.ds(row, 1), :]
        used = lax.broadcasted_iota(jnp.int32, (slots, LANES), 0) < counts[0, p]
        for h in range(halves):
            value = jnp.where(used, stage[h][...], 0.0)
            out[p, :, h * LANES : (h + 1) * LANES] = value.astype(BF16)
        pltpu.make_async_copy(out.at[p], out_in.at[p], sems.at[2 + parts]).start()

    pltpu.make_async_copy(out, out_in, sems.at[2 + parts]).wait()


def gather_rows(x, picks, counts):
    rows, width = x.shape
    peers, slots = picks.shape
    halves = width // LANES
    return pl.pallas_call(
        gather_kernel,
        out_shape=jax.ShapeDtypeStruct((peers, slots, width), BF16),
        in_specs=[ANY, ANY, ANY],
        out_specs=ANY,
        scratch_shapes=[
            pltpu.SMEM(picks.shape, jnp.int32),
            pltpu.SMEM(counts.shape, jnp.int32),
            pltpu.VMEM((rows, width), BF16),
            pltpu.VMEM((peers, slots, width), BF16),
            pltpu.SemaphoreType.DMA((7,)),
        ]
        + [pltpu.VMEM((rows, LANES), F32)] * halves
        + [pltpu.VMEM((slots, LANES), F32)] * halves,
        compiler_params=params(60),
        cost_estimate=cost(1e10, 4 * rows * width),
        name="gather_rows",
    )(picks, counts, x)


def local_kernel(src, dst, tiles, x, edge, edge_t, own_t, by_src, neigh, scale, order):
    count, tb, _ = tiles.shape
    own = neigh.shape[0]

    @pl.loop(0, count)
    def _(t):
        order[src[0, t]] = t

    neigh[...] = jnp.zeros_like(neigh)
    scale[...] = jnp.zeros_like(scale)
    ones = jnp.ones((8, tb), BF16)

    @pl.loop(0, own)
    def _(s):
        t = order[s]
        d = dst[0, t]
        by_src[s] = d
        tile = tiles[t].astype(F32)
        adj = tile.astype(BF16)
        own_t[s] = tile.T.astype(BF16)
        at = pl.ds(pl.multiple_of(s * tb, tb), tb)
        neigh[d] += matmul(adj, x[at, :])
        scale[d] += matmul_t(ones, adj)

    @pl.loop(own, count)
    def _(s):
        t = order[s]
        d = dst[0, t]
        by_src[s] = d
        tile = tiles[t].astype(F32)
        adj = tile.astype(BF16)
        edge[s - own] = adj
        edge_t[s - own] = tile.T.astype(BF16)
        scale[d] += matmul_t(ones, adj)

    scale[...] = 1.0 / (1.0 + scale[...])


def local_work(src, dst, tiles, x):
    count, tb, _ = tiles.shape
    rows, width = x.shape
    own = rows // tb
    edges = count - own
    return pl.pallas_call(
        local_kernel,
        out_shape=(
            jax.ShapeDtypeStruct((edges, tb, tb), BF16),
            jax.ShapeDtypeStruct((edges, tb, tb), BF16),
            jax.ShapeDtypeStruct((own, tb, tb), BF16),
            jax.ShapeDtypeStruct((count,), jnp.int32),
            jax.ShapeDtypeStruct((own, tb, width), F32),
            jax.ShapeDtypeStruct((own, 8, tb), F32),
        ),
        in_specs=[SMEM, SMEM, VMEM, VMEM],
        out_specs=(VMEM, VMEM, VMEM, SMEM, VMEM, VMEM),
        scratch_shapes=[pltpu.SMEM((count,), jnp.int32)],
        compiler_params=params(48),
        cost_estimate=cost(2e10, 4 * tiles.size),
        name="local_work",
    )(src, dst, tiles, x)


def spread_scale(scale, scale_v):
    own, _, tb = scale.shape

    @pl.loop(0, own, unroll=4)
    def _(s):
        scale_v[s] = jnp.broadcast_to(scale[s, 0:1, :], (tb, tb)).T


def rates_of(scale_v, which, size, width):
    rate = scale_v[which].reshape(size, scale_v.shape[2])
    return jnp.concatenate([rate] * (width // scale_v.shape[2]), 1)


def activation(x, agg, cot, w_self, w_neigh, bias):
    pre = matmul(x, w_self) + matmul(agg, w_neigh) + bias
    sig = 0.5 * jnp.tanh(0.5 * pre) + 0.5
    dpre = cot.astype(F32) * (sig * (1.0 + pre * (1.0 - sig)))
    return pre * sig, dpre


def middle_kernel(
    by_src, arrived, edge, edge_t, neigh, x, cot, scale, w_self, w_neigh, bias,
    agg_out, back_out,
    arrived_v, edge_v, edge_tv, product, acc, scale_v, x_v, cot_v, agg_v, g_v, back_v, sems,
):
    own, tb, width = acc.shape
    edges = product.shape[0]
    rows = own * tb
    parts = 4
    number = iter(range(sems.shape[0]))

    def start(source, target):
        copy = pltpu.make_async_copy(source, target, sems.at[next(number)])
        copy.start()
        return copy

    def cuts(size):
        return [pl.ds(c * (size // parts), size // parts) for c in range(parts)]

    def start_cuts(source, target, size):
        return [start(source.at[at], target.at[at]) for at in cuts(size)]

    coming = []
    for at in cuts(edges):
        coming.append(
            (start(edge.at[at], edge_v.at[at]), start(arrived.at[at], arrived_v.at[at]))
        )
    in_neigh = start(neigh, acc)
    nodes = start_cuts(x, x_v, rows)
    cots = start_cuts(cot, cot_v, rows)
    in_edge_t = start(edge_t, edge_tv)
    spread_scale(scale, scale_v)

    each = edges // parts
    for c in range(parts):
        for copy in coming[c]:
            copy.wait()

        @pl.loop(c * each, (c + 1) * each, unroll=4)
        def _(s):
            product[s] = matmul(edge_v[s], arrived_v[s])

    in_neigh.wait()

    @pl.loop(0, edges)
    def _(s):
        acc[by_src[own + s]] += product[s]

    block = 4
    size = block * tb
    leaving = []
    for c in range(parts):
        nodes[c].wait()
        cots[c].wait()

        @pl.loop(c * (own // parts) // block, (c + 1) * (own // parts) // block)
        def _(i):
            at = pl.ds(pl.multiple_of(i * size, size), size)
            which = pl.ds(i * block, block)
            rate = rates_of(scale_v, which, size, width)
            agg = (acc[which].reshape(size, width) * rate).astype(BF16)
            agg_v[at, :] = agg
            _, dpre = activation(
                x_v[at, :], agg, cot_v[at, :], w_self[...], w_neigh[...], bias[...]
            )
            g = (matmul_t(dpre.astype(BF16), w_neigh[...]) * rate).astype(BF16)
            g_v[which] = g.reshape(block, tb, width)

        at = cuts(rows)[c]
        leaving.append(start(agg_v.at[at], agg_out.at[at]))

    in_edge_t.wait()
    for c in range(parts):

        @pl.loop(c * each, (c + 1) * each, unroll=4)
        def _(s):
            back_v[s] = matmul(edge_tv[s], g_v[by_src[own + s]]).astype(BF16)

        at = cuts(edges)[c]
        leaving.append(start(back_v.at[at], back_out.at[at]))
    for copy in leaving:
        copy.wait()


def middle_work(by_src, arrived, edge, edge_t, neigh, x, cot, scale, w_self, w_neigh, bias):
    own, tb, width = neigh.shape
    edges = edge.shape[0]
    rows, hidden = cot.shape
    return pl.pallas_call(
        middle_kernel,
        out_shape=(
            jax.ShapeDtypeStruct((rows, width), BF16),
            jax.ShapeDtypeStruct((edges, tb, width), BF16),
        ),
        in_specs=[SMEM] + [ANY] * 6 + [VMEM] * 4,
        out_specs=(ANY, ANY),
        scratch_shapes=[
            pltpu.VMEM((edges, tb, width), BF16),
            pltpu.VMEM((edges, tb, tb), BF16),
            pltpu.VMEM((edges, tb, tb), BF16),
            pltpu.VMEM((edges, tb, width), F32),
            pltpu.VMEM((own, tb, width), F32),
            pltpu.VMEM((own, tb, tb), F32),
            pltpu.VMEM((rows, width), BF16),
            pltpu.VMEM((rows, hidden), BF16),
            pltpu.VMEM((rows, width), BF16),
            pltpu.VMEM((own, tb, width), BF16),
            pltpu.VMEM((edges, tb, width), BF16),
            pltpu.SemaphoreType.DMA((32,)),
        ],
        compiler_params=params(60),
        cost_estimate=cost(2e10, 16 * rows * width),
        name="middle_work",
    )(by_src, arrived, edge, edge_t, neigh, x, cot, scale, w_self, w_neigh, bias)


def tail_kernel(
    agg, x, cot, scale, w_self, w_neigh, bias, layer_out, dpre_out, g_out, terms, scale_v
):
    rows, width = x.shape
    own, tb, _ = g_out.shape
    hidden = cot.shape[1]
    spread_scale(scale, scale_v)
    terms[...] = jnp.zeros_like(terms)
    block = 4
    size = block * tb

    @pl.loop(0, own // block)
    def _(i):
        at = pl.ds(pl.multiple_of(i * size, size), size)
        which = pl.ds(i * block, block)
        near = agg[at, :]
        layer, dpre = activation(
            x[at, :], near, cot[at, :], w_self[...], w_neigh[...], bias[...]
        )
        layer_out[at, :] = layer.astype(BF16)
        dpre_b = dpre.astype(BF16)
        dpre_out[at, :] = dpre_b
        rate = rates_of(scale_v, which, size, width)
        g = (matmul_t(dpre_b, w_neigh[...]) * rate).astype(BF16)
        g_out[which] = g.reshape(block, tb, width)
        dims = (((0,), (0,)), ((), ()))
        terms[:width, :] += lax.dot_general(x[at, :], dpre_b, dims, preferred_element_type=F32)
        terms[width : 2 * width, :] += lax.dot_general(
            near, dpre_b, dims, preferred_element_type=F32
        )
        terms[2 * width : 2 * width + 8, :] += jnp.sum(dpre.reshape(size // 8, 8, hidden), axis=0)


def tail_work(agg, x, cot, scale, w_self, w_neigh, bias, spare):
    rows, width = x.shape
    own, _, tb = scale.shape
    hidden = cot.shape[1]
    return pl.pallas_call(
        tail_kernel,
        out_shape=(
            jax.ShapeDtypeStruct((rows, hidden), BF16),
            jax.ShapeDtypeStruct((rows, hidden), BF16),
            jax.ShapeDtypeStruct((own, tb, width), BF16),
            jax.ShapeDtypeStruct((2 * width + spare, hidden), F32),
        ),
        in_specs=[VMEM] * 7,
        out_specs=(VMEM,) * 4,
        scratch_shapes=[pltpu.VMEM((own, tb, tb), F32)],
        compiler_params=params(40),
        cost_estimate=cost(1e10, 16 * rows * width),
        name="tail_work",
    )(agg, x, cot, scale, w_self, w_neigh, bias)


def own_kernel(by_src, own_t, g, dpre_b, w_self, out):
    own, tb, width = g.shape

    @pl.loop(0, own, unroll=4)
    def _(s):
        at = pl.ds(pl.multiple_of(s * tb, tb), tb)
        back = matmul(own_t[s], g[by_src[s]])
        out[at, :] = back + matmul_t(dpre_b[at, :], w_self[...])


def own_work(by_src, own_t, g, dpre_b, w_self):
    own, tb, width = g.shape
    return pl.pallas_call(
        own_kernel,
        out_shape=jax.ShapeDtypeStruct((own * tb, width), F32),
        in_specs=[SMEM] + [VMEM] * 4,
        out_specs=VMEM,
        compiler_params=params(24),
        cost_estimate=cost(1e10, 10 * own * tb * width),
        name="own_work",
    )(by_src, own_t, g, dpre_b, w_self)


def scatter_kernel(picks, base, returned_in, out_in, returned, out, sems):
    rows, width = base.shape
    count = picks.shape[1]
    parts = 4
    depth = count // parts
    block = 512
    coming = []
    for c in range(parts):
        at = pl.ds(c * depth, depth)
        coming.append(pltpu.make_async_copy(returned_in.at[at], returned.at[at], sems.at[c]))
    for copy in coming:
        copy.start()
    for copy in coming:
        copy.wait()
    inner = 512

    def send(i):
        at = pl.ds(pl.multiple_of(i * block, block), block)
        return pltpu.make_async_copy(out.at[at], out_in.at[at], sems.at[parts])

    @pl.loop(0, rows // block)
    def _(i):
        at = pl.ds(pl.multiple_of(i * block, block), block)
        here = lax.broadcasted_iota(jnp.int32, (block, inner), 0) + i * block
        total = base[at, :]
        for k in range(count // inner):
            hit = here == picks[:, k * inner : (k + 1) * inner]
            hot = jnp.where(hit, 1.0, 0.0).astype(BF16)
            total += matmul(hot, returned[k * inner : (k + 1) * inner, :])
        out[at, :] = total
        send(i).start()

    pltpu.make_async_copy(out, out_in, sems.at[parts]).wait()


def scatter_rows(picks, base, returned):
    rows, width = base.shape
    return pl.pallas_call(
        scatter_kernel,
        out_shape=jax.ShapeDtypeStruct((rows, width), F32),
        in_specs=[VMEM, VMEM, ANY],
        out_specs=ANY,
        scratch_shapes=[
            pltpu.VMEM(returned.shape, BF16),
            pltpu.VMEM((rows, width), F32),
            pltpu.SemaphoreType.DMA((5,)),
        ],
        compiler_params=params(32),
        cost_estimate=cost(1e10, 10 * rows * width),
        name="scatter_rows",
    )(picks, base, returned)


def exchange(block, groups=None):
    return lax.all_to_all(block, AXES, 0, 0, tiled=True, axis_index_groups=groups)


def flip(value, bit, members):
    return lax.ppermute(value, AXES, [(i, i ^ bit) for i in range(members)])


def split_bits(shape):
    n_row, n_col = shape
    inner = n_col // 4 if n_col % 4 == 0 else n_col
    near = [1 << i for i in range(inner.bit_length() - 1)]
    near += [n_col << i for i in range(n_row.bit_length() - 1)]
    return near, [inner * i for i in range(1, n_col // inner)]


def share_of_total(terms, shape):
    members = shape[0] * shape[1]
    near, far = split_bits(shape)
    me = lax.axis_index(AXES)
    for bit in near:
        upper = (me & bit) != 0
        half = terms.shape[0] // 2
        low, high = terms[:half], terms[half:]
        terms = jnp.where(upper, high, low) + flip(jnp.where(upper, low, high), bit, members)
    levels = [terms] + [flip(terms, bits, members) for bits in far]
    while len(levels) > 1:
        levels = [levels[i] + levels[i + 1] for i in range(0, len(levels), 2)]
    return levels[0]


def join_shares(share, shape):
    members = shape[0] * shape[1]
    near, _ = split_bits(shape)

    def place(device):
        return sum(1 << (len(near) - 1 - i) for i, bit in enumerate(near) if device & bit)

    mask = sum(near)
    planes = {}
    for device in range(members):
        planes.setdefault(device & ~mask, []).append(device)
    groups = [sorted(plane, key=place) for _, plane in sorted(planes.items())]
    count = len(groups[0])
    whole = exchange(jnp.broadcast_to(share[None], (count,) + share.shape), groups)
    return whole.reshape(count * share.shape[0], share.shape[1])


def on_device(
    shape, features, send_rows, counts, tile_dst, tile_src, tiles, w_self, w_neigh, bias, cotangent
):
    rows, width = features.shape
    peers, slots = send_rows.shape[1:]
    picks = send_rows[0]
    outgoing = gather_rows(features, picks, counts)
    arrived = exchange(outgoing)
    edge, edge_t, own_t, by_src, neigh, scale = local_work(tile_src, tile_dst, tiles[0], features)
    keep = jnp.arange(slots, dtype=jnp.int32)[None, :] < counts[0][:, None]
    targets = jnp.where(keep, picks, -1).reshape(1, peers * slots)
    agg, back_b = middle_work(
        by_src, arrived, edge, edge_t, neigh, features, cotangent, scale, w_self, w_neigh, bias[None]
    )
    returned = exchange(back_b).reshape(peers * slots, width)
    spare = 8 << len(split_bits(shape)[0])
    layer_out, dpre_b, g, terms = tail_work(
        agg, features, cotangent, scale, w_self, w_neigh, bias[None], spare
    )
    own_grad = own_work(by_src, own_t, g, dpre_b, w_self)
    share = share_of_total(terms, shape)
    share, returned = lax.optimization_barrier((share, returned))
    terms = join_shares(share, shape)
    bias_total = jnp.sum(terms[2 * width : 2 * width + 8], axis=0)
    grad_features = scatter_rows(targets, own_grad, returned)
    inv_root = 1.0 / jnp.sqrt(F32(rows * shape[0] * shape[1]))
    return (
        layer_out,
        grad_features,
        terms[:width] * inv_root,
        terms[width : 2 * width] * inv_root,
        bias_total * inv_root,
    )


def solution(mesh):
    both = P(AXES)
    in_specs = (both,) * 6 + (P(),) * 3 + (both,)
    out_specs = (both, both, P(), P(), P())
    shape = (mesh.shape["row"], mesh.shape["col"])
    return jax.shard_map(
        functools.partial(on_device, shape),
        mesh=mesh,
        in_specs=in_specs,
        out_specs=out_specs,
        check_vma=False,
    )
```

```python
import functools

import jax
import jax.numpy as jnp
from jax import lax
from jax.experimental import pallas as pl
from jax.experimental.pallas import tpu as pltpu
from jax.sharding import PartitionSpec as P

AXES = ("row", "col")
LANES = 128
MIDDLE_MIB = 52
SCATTER_MIB = 52
VMEM = pl.BlockSpec(memory_space=pltpu.VMEM)
SMEM = pl.BlockSpec(memory_space=pltpu.SMEM)
ANY = pl.BlockSpec(memory_space=pl.ANY)
F32 = jnp.float32
BF16 = jnp.bfloat16


def matmul(a, b):
    return jnp.dot(a, b, preferred_element_type=F32)


def matmul_t(a, b):
    return lax.dot_general(a, b, (((1,), (1,)), ((), ())), preferred_element_type=F32)


def params(mib):
    return pltpu.CompilerParams(vmem_limit_bytes=int(mib * 1024 * 1024))


def cost(flops, nbytes):
    return pl.CostEstimate(flops=int(flops), bytes_accessed=int(nbytes), transcendentals=0)


def loosen(target, first, value):
    rows, width = value.shape
    halves = width // LANES
    for h in range(halves):
        at = pl.ds(first * halves + h, rows, stride=halves)
        target[at, :] = value[:, h * LANES : (h + 1) * LANES].astype(F32)


def tighten(source, first, rows, halves):
    parts = [source[pl.ds(first * halves + h, rows, stride=halves), :] for h in range(halves)]
    return jnp.concatenate(parts, 1)


def row_at(index, halves):
    return pl.ds(pl.multiple_of(index * halves, halves), halves)


def gather_kernel(picks_in, counts_in, x_in, out_in, picks, counts, x, out, wide, stage, sems):
    rows, width = x.shape
    peers, slots = picks.shape
    halves = width // LANES
    parts = 4
    chunk = rows // parts
    step = 128
    copies = [
        pltpu.make_async_copy(picks_in, picks, sems.at[0]),
        pltpu.make_async_copy(counts_in, counts, sems.at[1]),
    ]
    for c in range(parts):
        at = pl.ds(c * chunk, chunk)
        copies.append(pltpu.make_async_copy(x_in.at[at], x.at[at], sems.at[2 + c]))
    for copy in copies:
        copy.start()
    for c in range(parts):
        copies[2 + c].wait()

        @pl.loop(c * chunk // step, (c + 1) * chunk // step)
        def _(i):
            first = pl.multiple_of(i * step, step)
            loosen(wide, first, x[pl.ds(first, step), :])

    copies[0].wait()
    copies[1].wait()

    @pl.loop(0, peers)
    def _(p):
        for k in range(slots):
            stage[row_at(k, halves), :] = wide[row_at(picks[p, k], halves), :]
        used = lax.broadcasted_iota(jnp.int32, (slots, width), 0) < counts[0, p]
        out[p] = jnp.where(used, tighten(stage, 0, slots, halves), 0.0).astype(BF16)
        pltpu.make_async_copy(out.at[p], out_in.at[p], sems.at[2 + parts]).start()

    pltpu.make_async_copy(out, out_in, sems.at[2 + parts]).wait()


def gather_rows(x, picks, counts):
    rows, width = x.shape
    peers, slots = picks.shape
    halves = width // LANES
    return pl.pallas_call(
        gather_kernel,
        out_shape=jax.ShapeDtypeStruct((peers, slots, width), BF16),
        in_specs=[ANY, ANY, ANY],
        out_specs=ANY,
        scratch_shapes=[
            pltpu.SMEM(picks.shape, jnp.int32),
            pltpu.SMEM(counts.shape, jnp.int32),
            pltpu.VMEM((rows, width), BF16),
            pltpu.VMEM((peers, slots, width), BF16),
            pltpu.VMEM((rows * halves, LANES), F32),
            pltpu.VMEM((slots * halves, LANES), F32),
            pltpu.SemaphoreType.DMA((7,)),
        ],
        compiler_params=params(60),
        cost_estimate=cost(1e10, 4 * rows * width),
        name="gather_rows",
    )(picks, counts, x)


def local_kernel(src, dst, tiles, adj, edge_t, own_t, by_src, scale, order):
    count, tb, _ = tiles.shape
    own = own_t.shape[0]

    @pl.loop(0, count)
    def _(t):
        order[src[0, t]] = t

    scale[...] = jnp.zeros_like(scale)
    ones = jnp.ones((8, tb), BF16)

    def take(s, turned):
        t = order[s]
        d = dst[0, t]
        by_src[s] = d
        tile = tiles[t].astype(F32)
        straight = tile.astype(BF16)
        adj[s] = straight
        turned(tile.T.astype(BF16))
        scale[d] += matmul_t(ones, straight)

    @pl.loop(0, own, unroll=4)
    def _(s):
        def keep(value):
            own_t[s] = value

        take(s, keep)

    @pl.loop(own, count, unroll=4)
    def _(s):
        def keep(value):
            edge_t[s - own] = value

        take(s, keep)

    scale[...] = 1.0 / (1.0 + scale[...])


def local_work(src, dst, tiles, own):
    count, tb, _ = tiles.shape
    edges = count - own
    return pl.pallas_call(
        local_kernel,
        out_shape=(
            jax.ShapeDtypeStruct((count, tb, tb), BF16),
            jax.ShapeDtypeStruct((edges, tb, tb), BF16),
            jax.ShapeDtypeStruct((own, tb, tb), BF16),
            jax.ShapeDtypeStruct((count,), jnp.int32),
            jax.ShapeDtypeStruct((own, 8, tb), F32),
        ),
        in_specs=[SMEM, SMEM, VMEM],
        out_specs=(VMEM, VMEM, VMEM, SMEM, VMEM),
        scratch_shapes=[pltpu.SMEM((count,), jnp.int32)],
        compiler_params=params(48),
        cost_estimate=cost(2e10, 4 * tiles.size),
        name="local_work",
    )(src, dst, tiles)


def spread_scale(scale, scale_v):
    own, _, tb = scale.shape

    @pl.loop(0, own, unroll=4)
    def _(s):
        scale_v[s] = jnp.broadcast_to(scale[s, 0:1, :], (tb, tb)).T


def rates_of(scale_v, which, size, width):
    rate = scale_v[which].reshape(size, scale_v.shape[2])
    return jnp.concatenate([rate] * (width // scale_v.shape[2]), 1)


def activation(x, agg, cot, w_self, w_neigh, bias):
    pre = matmul(x, w_self) + matmul(agg, w_neigh) + bias
    sig = 0.5 * jnp.tanh(0.5 * pre) + 0.5
    dpre = cot.astype(F32) * (sig * (1.0 + pre * (1.0 - sig)))
    return pre * sig, dpre


def middle_kernel(
    by_src, arrived, adj, edge_t, x, cot, scale, w_self, w_neigh, bias,
    agg_out, back_out,
    arrived_v, adj_v, edge_tv, acc, scale_v, x_v, cot_v, agg_v, g_v, back_v, sems,
):
    own, tb, width = acc.shape
    edges = edge_tv.shape[0]
    rows = own * tb
    parts = 4
    number = iter(range(sems.shape[0]))

    def start(source, target):
        copy = pltpu.make_async_copy(source, target, sems.at[next(number)])
        copy.start()
        return copy

    def cuts(size):
        return [pl.ds(c * (size // parts), size // parts) for c in range(parts)]

    def start_cuts(source, target, size):
        return [start(source.at[at], target.at[at]) for at in cuts(size)]

    coming = []
    for first, size, source, target in ((own, edges, arrived, arrived_v), (0, own, x, x_v)):
        each = size // parts
        unit = target.shape[0] // parts
        for c in range(parts):
            tiles = pl.ds(first + c * each, each)
            at = pl.ds(c * unit, unit)
            needs = start(adj.at[tiles], adj_v.at[tiles]), start(source.at[at], target.at[at])
            coming.append((first + c * each, each, needs))
    cots = start_cuts(cot, cot_v, rows)
    in_edge_t = start(edge_t, edge_tv)
    acc[...] = jnp.zeros_like(acc)
    spread_scale(scale, scale_v)

    for first, each, needs in coming:
        for copy in needs:
            copy.wait()

        @pl.loop(0, each, unroll=8)
        def _(i):
            s = first + i
            if first < own:
                block = x_v[pl.ds(pl.multiple_of(s * tb, tb), tb), :]
            else:
                block = arrived_v[s - own]
            acc[by_src[s]] += matmul(adj_v[s], block)

    each = edges // parts
    block = min(8, own // parts)
    size = block * tb
    leaving = []
    for c in range(parts):
        cots[c].wait()

        @pl.loop(c * (own // parts) // block, (c + 1) * (own // parts) // block)
        def _(i):
            at = pl.ds(pl.multiple_of(i * size, size), size)
            which = pl.ds(i * block, block)
            rate = rates_of(scale_v, which, size, width)
            agg = (acc[which].reshape(size, width) * rate).astype(BF16)
            agg_v[at, :] = agg
            _, dpre = activation(
                x_v[at, :], agg, cot_v[at, :], w_self[...], w_neigh[...], bias[...]
            )
            g = (matmul_t(dpre.astype(BF16), w_neigh[...]) * rate).astype(BF16)
            g_v[which] = g.reshape(block, tb, width)

        at = cuts(rows)[c]
        leaving.append(start(agg_v.at[at], agg_out.at[at]))

    in_edge_t.wait()
    for c in range(parts):

        @pl.loop(c * each, (c + 1) * each, unroll=8)
        def _(s):
            back_v[s] = matmul(edge_tv[s], g_v[by_src[own + s]]).astype(BF16)

        at = cuts(edges)[c]
        leaving.append(start(back_v.at[at], back_out.at[at]))
    for copy in leaving:
        copy.wait()


def middle_work(by_src, arrived, adj, edge_t, x, cot, scale, w_self, w_neigh, bias):
    edges, tb, width = arrived.shape
    own = scale.shape[0]
    rows, hidden = cot.shape
    return pl.pallas_call(
        middle_kernel,
        out_shape=(
            jax.ShapeDtypeStruct((rows, width), BF16),
            jax.ShapeDtypeStruct((edges, tb, width), BF16),
        ),
        in_specs=[SMEM] + [ANY] * 5 + [VMEM] * 4,
        out_specs=(ANY, ANY),
        scratch_shapes=[
            pltpu.VMEM((edges, tb, width), BF16),
            pltpu.VMEM((own + edges, tb, tb), BF16),
            pltpu.VMEM((edges, tb, tb), BF16),
            pltpu.VMEM((own, tb, width), F32),
            pltpu.VMEM((own, tb, tb), F32),
            pltpu.VMEM((rows, width), BF16),
            pltpu.VMEM((rows, hidden), BF16),
            pltpu.VMEM((rows, width), BF16),
            pltpu.VMEM((own, tb, width), BF16),
            pltpu.VMEM((edges, tb, width), BF16),
            pltpu.SemaphoreType.DMA((32,)),
        ],
        compiler_params=params(MIDDLE_MIB),
        cost_estimate=cost(2e10, 16 * rows * width),
        name="middle_work",
    )(by_src, arrived, adj, edge_t, x, cot, scale, w_self, w_neigh, bias)


def tail_kernel(
    agg_in, x_in, cot_in, scale, w_self, w_neigh, bias,
    layer_out, dpre_out, g_out, terms,
    agg, x, cot, layer_v, dpre_v, g_v, scale_v, sems,
):
    rows, width = x.shape
    own, tb, _ = g_v.shape
    hidden = cot.shape[1]
    block = 4
    size = block * tb
    steps = own // block
    sources = ((agg_in, agg), (x_in, x), (cot_in, cot))

    def at_step(i):
        return pl.ds(i * size, size), pl.ds(i * block, block)

    def fetch(i):
        at, _ = at_step(i)
        return [
            pltpu.make_async_copy(source.at[at], target.at[at], sems.at[3 * i + n])
            for n, (source, target) in enumerate(sources)
        ]

    for i in range(steps):
        for copy in fetch(i):
            copy.start()
    spread_scale(scale, scale_v)
    terms[...] = jnp.zeros_like(terms)
    leaving = []
    for i in range(steps):
        at, which = at_step(i)
        for copy in fetch(i):
            copy.wait()
        near = agg[at, :]
        layer, dpre = activation(
            x[at, :], near, cot[at, :], w_self[...], w_neigh[...], bias[...]
        )
        layer_v[at, :] = layer.astype(BF16)
        dpre_b = dpre.astype(BF16)
        dpre_v[at, :] = dpre_b
        rate = rates_of(scale_v, which, size, width)
        g = (matmul_t(dpre_b, w_neigh[...]) * rate).astype(BF16)
        g_v[which] = g.reshape(block, tb, width)
        dims = (((0,), (0,)), ((), ()))
        terms[:width, :] += lax.dot_general(x[at, :], dpre_b, dims, preferred_element_type=F32)
        terms[width : 2 * width, :] += lax.dot_general(
            near, dpre_b, dims, preferred_element_type=F32
        )
        terms[2 * width : 2 * width + 8, :] += jnp.sum(dpre.reshape(size // 8, 8, hidden), axis=0)
        for n, (source, target) in enumerate(
            (
                (layer_v.at[at], layer_out.at[at]),
                (dpre_v.at[at], dpre_out.at[at]),
                (g_v.at[which], g_out.at[which]),
            )
        ):
            copy = pltpu.make_async_copy(source, target, sems.at[3 * (steps + i) + n])
            copy.start()
            leaving.append(copy)
    for copy in leaving:
        copy.wait()


def tail_work(agg, x, cot, scale, w_self, w_neigh, bias, spare):
    rows, width = x.shape
    own, _, tb = scale.shape
    hidden = cot.shape[1]
    return pl.pallas_call(
        tail_kernel,
        out_shape=(
            jax.ShapeDtypeStruct((rows, hidden), BF16),
            jax.ShapeDtypeStruct((rows, hidden), BF16),
            jax.ShapeDtypeStruct((own, tb, width), BF16),
            jax.ShapeDtypeStruct((2 * width + spare, hidden), F32),
        ),
        in_specs=[ANY] * 3 + [VMEM] * 4,
        out_specs=(ANY, ANY, ANY, VMEM),
        scratch_shapes=[
            pltpu.VMEM((rows, width), BF16),
            pltpu.VMEM((rows, width), BF16),
            pltpu.VMEM((rows, hidden), BF16),
            pltpu.VMEM((rows, hidden), BF16),
            pltpu.VMEM((rows, hidden), BF16),
            pltpu.VMEM((own, tb, width), BF16),
            pltpu.VMEM((own, tb, tb), F32),
            pltpu.SemaphoreType.DMA((6 * (own // 4),)),
        ],
        compiler_params=params(62.5),
        cost_estimate=cost(1e10, 16 * rows * width),
        name="tail_work",
    )(agg, x, cot, scale, w_self, w_neigh, bias)


def own_kernel(by_src, own_t, g, dpre_b, w_self, out):
    own, tb, width = g.shape

    @pl.loop(0, own, unroll=4)
    def _(s):
        at = pl.ds(pl.multiple_of(s * tb, tb), tb)
        back = matmul(own_t[s], g[by_src[s]])
        out[at, :] = back + matmul_t(dpre_b[at, :], w_self[...])


def own_work(by_src, own_t, g, dpre_b, w_self):
    own, tb, width = g.shape
    return pl.pallas_call(
        own_kernel,
        out_shape=jax.ShapeDtypeStruct((own * tb, width), F32),
        in_specs=[SMEM] + [VMEM] * 4,
        out_specs=VMEM,
        compiler_params=params(24),
        cost_estimate=cost(1e10, 10 * own * tb * width),
        name="own_work",
    )(by_src, own_t, g, dpre_b, w_self)


def scatter_kernel(
    targets_in, base_in, returned_in, out_in, targets, base, returned, out, stage, sems, *sums
):
    rows, width = base.shape
    peers, slots = targets.shape
    halves = width // LANES
    copies = [
        pltpu.make_async_copy(targets_in, targets, sems.at[0]),
        pltpu.make_async_copy(base_in, base, sems.at[1]),
    ]
    parts = 4
    each = peers // parts
    for c in range(parts):
        at = pl.ds(c * each, each)
        copies.append(pltpu.make_async_copy(returned_in.at[at], returned.at[at], sems.at[3 + c]))
    copies.append(copies.pop(1))
    for copy in copies:
        copy.start()
    for total in sums:
        total[...] = jnp.zeros_like(total)
    copies[0].wait()

    for c in range(parts):
        copies[1 + c].wait()

        @pl.loop(c * each, (c + 1) * each)
        def _(p):
            loosen(stage, 0, returned[p])
            for k in range(0, slots, len(sums)):
                places = [row_at(targets[p, k + j], halves) for j in range(len(sums))]
                values = [
                    total[place, :] + stage[row_at(k + j, halves), :]
                    for j, (total, place) in enumerate(zip(sums, places))
                ]
                for total, place, value in zip(sums, places, values):
                    total[place, :] = value

    copies[1 + parts].wait()
    block = 256

    @pl.loop(0, rows // block)
    def _(i):
        first = pl.multiple_of(i * block, block)
        at = pl.ds(first, block)
        value = base[at, :]
        for total in sums:
            value += tighten(total, first, block, halves)
        out[at, :] = value
        pltpu.make_async_copy(out.at[at], out_in.at[at], sems.at[2]).start()

    pltpu.make_async_copy(out, out_in, sems.at[2]).wait()


def scatter_rows(targets, base, returned):
    rows, width = base.shape
    peers, slots = targets.shape
    halves = width // LANES
    return pl.pallas_call(
        scatter_kernel,
        out_shape=jax.ShapeDtypeStruct((rows, width), F32),
        in_specs=[ANY, ANY, ANY],
        out_specs=ANY,
        scratch_shapes=[
            pltpu.SMEM(targets.shape, jnp.int32),
            pltpu.VMEM((rows, width), F32),
            pltpu.VMEM((peers, slots, width), BF16),
            pltpu.VMEM((rows, width), F32),
            pltpu.VMEM((slots * halves, LANES), F32),
            pltpu.SemaphoreType.DMA((7,)),
        ]
        + [pltpu.VMEM(((rows + 8) * halves, LANES), F32)] * 4,
        compiler_params=params(SCATTER_MIB),
        cost_estimate=cost(1e10, 10 * rows * width),
        name="scatter_rows",
    )(targets, base, returned)


def exchange(block, groups=None):
    return lax.all_to_all(block, AXES, 0, 0, tiled=True, axis_index_groups=groups)


def flip(value, bit, members):
    return lax.ppermute(value, AXES, [(i, i ^ bit) for i in range(members)])


def split_bits(shape):
    n_row, n_col = shape
    inner = n_col // 4 if n_col % 4 == 0 else n_col
    near = [1 << i for i in range(inner.bit_length() - 1)]
    near += [n_col << i for i in range(n_row.bit_length() - 1)]
    return near, [inner << i for i in range((n_col // inner).bit_length() - 1)]


def share_of_total(terms, shape):
    members = shape[0] * shape[1]
    near, far = split_bits(shape)
    me = lax.axis_index(AXES)
    for bit in near:
        upper = (me & bit) != 0
        half = terms.shape[0] // 2
        low, high = terms[:half], terms[half:]
        terms = jnp.where(upper, high, low) + flip(jnp.where(upper, low, high), bit, members)
    for bit in far:
        terms = terms + flip(terms, bit, members)
    return terms


def share_groups(shape):
    members = shape[0] * shape[1]
    near, _ = split_bits(shape)

    def place(device):
        return sum(1 << (len(near) - 1 - i) for i, bit in enumerate(near) if device & bit)

    mask = sum(near)
    planes = {}
    for device in range(members):
        planes.setdefault(device & ~mask, []).append(device)
    groups = [sorted(plane, key=place) for _, plane in sorted(planes.items())]
    return groups


def on_device(
    shape, features, send_rows, counts, tile_dst, tile_src, tiles, w_self, w_neigh, bias, cotangent
):
    rows, width = features.shape
    peers, slots = send_rows.shape[1:]
    picks = send_rows[0]
    outgoing = gather_rows(features, picks, counts)
    arrived = exchange(outgoing)
    adj, edge_t, own_t, by_src, scale = local_work(tile_src, tile_dst, tiles[0], rows // slots)
    keep = jnp.arange(slots, dtype=jnp.int32)[None, :] < counts[0][:, None]
    targets = jnp.where(keep, picks, rows)
    agg, back_b = middle_work(
        by_src, arrived, adj, edge_t, features, cotangent, scale, w_self, w_neigh, bias[None]
    )
    returned = exchange(back_b)
    spare = 8 << len(split_bits(shape)[0])
    layer_out, dpre_b, g, terms = tail_work(
        agg, features, cotangent, scale, w_self, w_neigh, bias[None], spare
    )
    own_grad = own_work(by_src, own_t, g, dpre_b, w_self)
    inv_root = 1.0 / jnp.sqrt(F32(rows * shape[0] * shape[1]))
    share = share_of_total(terms, shape) * inv_root
    groups = share_groups(shape)
    packed = jnp.broadcast_to(share[None], (len(groups[0]),) + share.shape)
    packed, returned = lax.optimization_barrier((packed, returned))
    terms = exchange(packed, groups).reshape(terms.shape)
    grad_features = scatter_rows(targets, own_grad, returned)
    grad_bias = jnp.sum(terms[2 * width : 2 * width + 8], axis=0)
    return layer_out, grad_features, terms[:width], terms[width : 2 * width], grad_bias


def solution(mesh):
    both = P(AXES)
    in_specs = (both,) * 6 + (P(),) * 3 + (both,)
    out_specs = (both, both, P(), P(), P())
    shape = (mesh.shape["row"], mesh.shape["col"])
    return jax.shard_map(
        functools.partial(on_device, shape),
        mesh=mesh,
        in_specs=in_specs,
        out_specs=out_specs,
        check_vma=False,
    )
```

```python
import functools

import jax
import jax.numpy as jnp
from jax import lax
from jax.experimental import pallas as pl
from jax.experimental.pallas import tpu as pltpu
from jax.sharding import PartitionSpec as P


AXES = ("row", "col")
LANES = 128
MOST_APART = 32
MIDDLE_MIB = 52
SCATTER_MIB = 52
VMEM = pl.BlockSpec(memory_space=pltpu.VMEM)
SMEM = pl.BlockSpec(memory_space=pltpu.SMEM)
ANY = pl.BlockSpec(memory_space=pl.ANY)
F32 = jnp.float32
BF16 = jnp.bfloat16


def matmul(a, b):
    return jnp.dot(a, b, preferred_element_type=F32)


def matmul_t(a, b):
    return lax.dot_general(a, b, (((1,), (1,)), ((), ())), preferred_element_type=F32)


def params(mib):
    return pltpu.CompilerParams(vmem_limit_bytes=int(mib * 1024 * 1024))


def cost(flops, nbytes):
    return pl.CostEstimate(flops=int(flops), bytes_accessed=int(nbytes), transcendentals=0)


def loosen(target, first, value):
    rows, width = value.shape
    halves = width // LANES
    for h in range(halves):
        at = pl.ds(first * halves + h, rows, stride=halves)
        target[at, :] = value[:, h * LANES : (h + 1) * LANES].astype(F32)


def tighten(source, first, rows, halves):
    parts = [source[pl.ds(first * halves + h, rows, stride=halves), :] for h in range(halves)]
    return jnp.concatenate(parts, 1)


def row_at(index, halves):
    return pl.ds(pl.multiple_of(index * halves, halves), halves)


def near_peer(me, far_bit, j):
    low = j & (far_bit - 1)
    return 2 * (j - low) + low + (me & far_bit)


def far_mask(far_bit, j):
    low = j & (far_bit - 1)
    return 2 * (j - low) + low + far_bit


def my_number(n_col):
    return lax.axis_index("row") * n_col + lax.axis_index("col")


def gather_kernel(whom, n_col, groups, picks_in, counts_in, x_in, *rest):
    outs, (picks, counts, x, out, wide, stage, sems) = rest[:-7], rest[-7:]
    me = my_number(n_col)
    rows, width = x.shape
    peers = out.shape[0]
    slots = picks.shape[1]
    halves = width // LANES
    parts = 4
    chunk = rows // parts
    step = 128
    copies = [
        pltpu.make_async_copy(picks_in, picks, sems.at[0]),
        pltpu.make_async_copy(counts_in, counts, sems.at[1]),
    ]
    for c in range(parts):
        at = pl.ds(c * chunk, chunk)
        copies.append(pltpu.make_async_copy(x_in.at[at], x.at[at], sems.at[2 + c]))
    for copy in copies:
        copy.start()
    for c in range(parts):
        copies[2 + c].wait()

        @pl.loop(c * chunk // step, (c + 1) * chunk // step)
        def _(i):
            first = pl.multiple_of(i * step, step)
            loosen(wide, first, x[pl.ds(first, step), :])

    copies[0].wait()
    copies[1].wait()

    each = peers // groups
    for c in range(groups):

        @pl.loop(c * each, (c + 1) * each)
        def _(j):
            p = whom(me, j)
            for k in range(slots):
                stage[row_at(k, halves), :] = wide[row_at(picks[p, k], halves), :]
            used = lax.broadcasted_iota(jnp.int32, (slots, width), 0) < counts[0, p]
            out[j] = jnp.where(used, tighten(stage, 0, slots, halves), 0.0).astype(BF16)

        if len(outs) == 1:
            at = pl.ds(c * each, each)
            pltpu.make_async_copy(out.at[at], outs[0].at[at], sems.at[6]).start()
        else:
            for j in range(c * each, (c + 1) * each):
                pltpu.make_async_copy(out.at[j], outs[j // 2].at[j % 2], sems.at[6]).start()

    if len(outs) == 1:
        pltpu.make_async_copy(out, outs[0], sems.at[6]).wait()
    else:
        for j in range(peers):
            pltpu.make_async_copy(out.at[j], outs[j // 2].at[j % 2], sems.at[6]).wait()


def gather_rows(x, picks, counts, whom, n_col, peers, apart):
    rows, width = x.shape
    slots = picks.shape[1]
    halves = width // LANES
    if apart:
        out_shape = (jax.ShapeDtypeStruct((2, slots, width), BF16),) * (peers // 2)
    else:
        out_shape = (jax.ShapeDtypeStruct((peers, slots, width), BF16),)
    return pl.pallas_call(
        functools.partial(gather_kernel, whom, n_col, min(4, peers // 2)),
        out_shape=out_shape,
        in_specs=[ANY, ANY, ANY],
        out_specs=(ANY,) * len(out_shape),
        scratch_shapes=[
            pltpu.SMEM(picks.shape, jnp.int32),
            pltpu.SMEM(counts.shape, jnp.int32),
            pltpu.VMEM((rows, width), BF16),
            pltpu.VMEM((peers, slots, width), BF16),
            pltpu.VMEM((rows * halves, LANES), F32),
            pltpu.VMEM((slots * halves, LANES), F32),
            pltpu.SemaphoreType.DMA((7,)),
        ],
        compiler_params=params(60),
        cost_estimate=cost(1e9, 4 * rows * width),
        name="gather_rows",
    )(picks, counts, x)


def peer_at(me, far_bit, peers, i):
    if not far_bit:
        return i
    half = peers // 2
    far = me ^ far_mask(far_bit, i - half)
    return jnp.where(i < half, near_peer(me, far_bit, i), far)


def local_kernel(n_col, far_bit, src, dst, tiles, adj, edge_t, own_t, by_src, by_turn, scale, order):
    count, tb, _ = tiles.shape
    own = own_t.shape[0]
    me = my_number(n_col)

    @pl.loop(0, count)
    def _(t):
        order[src[0, t]] = t

    scale[...] = jnp.zeros_like(scale)
    ones = jnp.ones((8, tb), BF16)

    def take(turn, s):
        t = order[s]
        d = dst[0, t]
        by_src[s] = d
        by_turn[turn] = d
        tile = tiles[t].astype(F32)
        straight = tile.astype(BF16)
        adj[turn] = straight
        scale[d] += matmul_t(ones, straight)
        return tile.T.astype(BF16)

    @pl.loop(0, own, unroll=4)
    def _(s):
        own_t[s] = take(s, s)

    @pl.loop(0, count - own, unroll=4)
    def _(i):
        p = peer_at(me, far_bit, count - own, i)
        edge_t[p] = take(own + i, own + p)

    scale[...] = 1.0 / (1.0 + scale[...])


def local_work(src, dst, tiles, own, n_col, far_bit):
    count, tb, _ = tiles.shape
    edges = count - own
    return pl.pallas_call(
        functools.partial(local_kernel, n_col, far_bit),
        out_shape=(
            jax.ShapeDtypeStruct((count, tb, tb), BF16),
            jax.ShapeDtypeStruct((edges, tb, tb), BF16),
            jax.ShapeDtypeStruct((own, tb, tb), BF16),
            jax.ShapeDtypeStruct((count,), jnp.int32),
            jax.ShapeDtypeStruct((count,), jnp.int32),
            jax.ShapeDtypeStruct((own, 8, tb), F32),
        ),
        in_specs=[SMEM, SMEM, VMEM],
        out_specs=(VMEM, VMEM, VMEM, SMEM, SMEM, VMEM),
        scratch_shapes=[pltpu.SMEM((count,), jnp.int32)],
        compiler_params=params(48),
        cost_estimate=cost(2e10, 4 * tiles.size),
        name="local_work",
    )(src, dst, tiles)


def spread_scale(scale, scale_v):
    own, _, tb = scale.shape

    @pl.loop(0, own, unroll=4)
    def _(s):
        scale_v[s] = jnp.broadcast_to(scale[s, 0:1, :], (tb, tb)).T


def rates_of(scale_v, which, size, width):
    rate = scale_v[which].reshape(size, scale_v.shape[2])
    return jnp.concatenate([rate] * (width // scale_v.shape[2]), 1)


def activation(x, agg, cot, w_self, w_neigh, bias):
    pre = matmul(x, w_self) + matmul(agg, w_neigh) + bias
    sig = 0.5 * jnp.tanh(0.5 * pre) + 0.5
    dpre = cot.astype(F32) * (sig * (1.0 + pre * (1.0 - sig)))
    return pre * sig, dpre


def middle_kernel(far_count, *refs):
    far, refs = refs[:far_count], refs[far_count:]
    pairs = far_count // 2
    (
        by_src, by_turn, near_in, adj, edge_t, x, cot, scale, w_self, w_neigh, bias,
        agg_out, back_out,
        near, adj_v, edge_tv, acc, scale_v, x_v, cot_v, agg_v, g_v, back_v, sems,
    ) = refs
    own, tb, width = acc.shape
    edges = edge_tv.shape[0]
    rows = own * tb
    parts = 4
    number = iter(range(sems.shape[0]))

    def start(source, target):
        copy = pltpu.make_async_copy(source, target, sems.at[next(number)])
        copy.start()
        return copy

    def cuts(size):
        return [pl.ds(c * (size // parts), size // parts) for c in range(parts)]

    def start_cuts(source, target, size):
        return [start(source.at[at], target.at[at]) for at in cuts(size)]

    near_count = near.shape[0]

    def own_tile(j):
        return x_v[pl.ds(pl.multiple_of(j * tb, tb), tb), :]

    def fetch_tiles(first, size):
        at = pl.ds(first, size)
        return start(adj.at[at], adj_v.at[at])

    coming = []
    each = own // parts
    for c, at in enumerate(cuts(rows)):
        needs = [fetch_tiles(c * each, each), start(x.at[at], x_v.at[at])]
        coming.append((own_tile, 0, c * each, each, needs))
    each = near_count // 2
    for c in range(2):
        at = pl.ds(c * each, each)
        needs = [fetch_tiles(own + c * each, each), start(near_in.at[at], near.at[at])]
        coming.append((near.__getitem__, own, c * each, each, needs))
    far_in = [fetch_tiles(own + near_count, far_count)] if far_count else []
    cots = start_cuts(cot, cot_v, rows)
    in_edge_t = start(edge_t, edge_tv)
    acc[...] = jnp.zeros_like(acc)
    spread_scale(scale, scale_v)

    for rows_of, base, first, each, needs in coming:
        for copy in needs:
            copy.wait()

        @pl.loop(first, first + each, unroll=8)
        def _(j):
            acc[by_turn[base + j]] += matmul(adj_v[base + j], rows_of(j))

    for copy in far_in:
        copy.wait()
    for i in range(far_count):
        s = own + near_count + i
        acc[by_turn[s]] += matmul(adj_v[s], far[i // 2 + (i % 2) * pairs][i % 2])

    each = edges // parts
    block = min(8, own // parts)
    size = block * tb
    leaving = []
    for c in range(parts):
        cots[c].wait()

        @pl.loop(c * (own // parts) // block, (c + 1) * (own // parts) // block)
        def _(i):
            at = pl.ds(pl.multiple_of(i * size, size), size)
            which = pl.ds(i * block, block)
            rate = rates_of(scale_v, which, size, width)
            agg = (acc[which].reshape(size, width) * rate).astype(BF16)
            agg_v[at, :] = agg
            _, dpre = activation(
                x_v[at, :], agg, cot_v[at, :], w_self[...], w_neigh[...], bias[...]
            )
            g = (matmul_t(dpre.astype(BF16), w_neigh[...]) * rate).astype(BF16)
            g_v[which] = g.reshape(block, tb, width)

        at = cuts(rows)[c]
        leaving.append(start(agg_v.at[at], agg_out.at[at]))

    in_edge_t.wait()
    for c in range(parts):

        @pl.loop(c * each, (c + 1) * each, unroll=8)
        def _(s):
            back_v[s] = matmul(edge_tv[s], g_v[by_src[own + s]]).astype(BF16)

        at = cuts(edges)[c]
        leaving.append(start(back_v.at[at], back_out.at[at]))
    for copy in leaving:
        copy.wait()


def middle_work(far, near, by_src, by_turn, adj, edge_t, x, cot, scale, w_self, w_neigh, bias):
    edges, tb, _ = edge_t.shape
    width = x.shape[1]
    own = scale.shape[0]
    rows, hidden = cot.shape
    return pl.pallas_call(
        functools.partial(middle_kernel, len(far)),
        out_shape=(
            jax.ShapeDtypeStruct((rows, width), BF16),
            jax.ShapeDtypeStruct((edges, tb, width), BF16),
        ),
        in_specs=[VMEM] * len(far) + [SMEM] * 2 + [ANY] * 5 + [VMEM] * 4,
        out_specs=(ANY, ANY),
        scratch_shapes=[
            pltpu.VMEM(near.shape, BF16),
            pltpu.VMEM((own + edges, tb, tb), BF16),
            pltpu.VMEM((edges, tb, tb), BF16),
            pltpu.VMEM((own, tb, width), F32),
            pltpu.VMEM((own, tb, tb), F32),
            pltpu.VMEM((rows, width), BF16),
            pltpu.VMEM((rows, hidden), BF16),
            pltpu.VMEM((rows, width), BF16),
            pltpu.VMEM((own, tb, width), BF16),
            pltpu.VMEM((edges, tb, width), BF16),
            pltpu.SemaphoreType.DMA((80,)),
        ],
        compiler_params=params(MIDDLE_MIB),
        cost_estimate=cost(2e10, 16 * rows * width),
        name="middle_work",
    )(*far, by_src, by_turn, near, adj, edge_t, x, cot, scale, w_self, w_neigh, bias)


def tail_kernel(
    agg_in, x_in, cot_in, scale, w_self, w_neigh, bias,
    layer_out, dpre_out, g_out, terms,
    agg, x, cot, layer_v, dpre_v, g_v, scale_v, sems,
):
    _, width = x.shape
    own, tb, _ = g_v.shape
    hidden = cot.shape[1]
    block = 4
    size = block * tb
    steps = own // block
    sources = ((agg_in, agg), (x_in, x), (cot_in, cot))

    def at_step(i):
        return pl.ds(i * size, size), pl.ds(i * block, block)

    def fetch(i):
        at, _ = at_step(i)
        return [
            pltpu.make_async_copy(source.at[at], target.at[at], sems.at[3 * i + n])
            for n, (source, target) in enumerate(sources)
        ]

    for i in range(steps):
        for copy in fetch(i):
            copy.start()
    spread_scale(scale, scale_v)
    terms[...] = jnp.zeros_like(terms)
    leaving = []
    for i in range(steps):
        at, which = at_step(i)
        for copy in fetch(i):
            copy.wait()
        near = agg[at, :]
        layer, dpre = activation(
            x[at, :], near, cot[at, :], w_self[...], w_neigh[...], bias[...]
        )
        layer_v[at, :] = layer.astype(BF16)
        dpre_b = dpre.astype(BF16)
        dpre_v[at, :] = dpre_b
        rate = rates_of(scale_v, which, size, width)
        g = (matmul_t(dpre_b, w_neigh[...]) * rate).astype(BF16)
        g_v[which] = g.reshape(block, tb, width)
        dims = (((0,), (0,)), ((), ()))
        terms[:width, :] += lax.dot_general(x[at, :], dpre_b, dims, preferred_element_type=F32)
        terms[width : 2 * width, :] += lax.dot_general(
            near, dpre_b, dims, preferred_element_type=F32
        )
        terms[2 * width : 2 * width + 8, :] += jnp.sum(dpre.reshape(size // 8, 8, hidden), axis=0)
        for n, (source, target) in enumerate(
            (
                (layer_v.at[at], layer_out.at[at]),
                (dpre_v.at[at], dpre_out.at[at]),
                (g_v.at[which], g_out.at[which]),
            )
        ):
            copy = pltpu.make_async_copy(source, target, sems.at[3 * (steps + i) + n])
            copy.start()
            leaving.append(copy)
    for copy in leaving:
        copy.wait()


def tail_work(agg, x, cot, scale, w_self, w_neigh, bias, spare):
    rows, width = x.shape
    own, _, tb = scale.shape
    hidden = cot.shape[1]
    return pl.pallas_call(
        tail_kernel,
        out_shape=(
            jax.ShapeDtypeStruct((rows, hidden), BF16),
            jax.ShapeDtypeStruct((rows, hidden), BF16),
            jax.ShapeDtypeStruct((own, tb, width), BF16),
            jax.ShapeDtypeStruct((2 * width + spare, hidden), F32),
        ),
        in_specs=[ANY] * 3 + [VMEM] * 4,
        out_specs=(ANY, ANY, ANY, VMEM),
        scratch_shapes=[
            pltpu.VMEM((rows, width), BF16),
            pltpu.VMEM((rows, width), BF16),
            pltpu.VMEM((rows, hidden), BF16),
            pltpu.VMEM((rows, hidden), BF16),
            pltpu.VMEM((rows, hidden), BF16),
            pltpu.VMEM((own, tb, width), BF16),
            pltpu.VMEM((own, tb, tb), F32),
            pltpu.SemaphoreType.DMA((6 * (own // 4),)),
        ],
        compiler_params=params(62.5),
        cost_estimate=cost(1e10, 16 * rows * width),
        name="tail_work",
    )(agg, x, cot, scale, w_self, w_neigh, bias)


def own_kernel(by_src, own_t, g, dpre_b, w_self, out):
    own, tb, _ = g.shape

    @pl.loop(0, own, unroll=4)
    def _(s):
        at = pl.ds(pl.multiple_of(s * tb, tb), tb)
        back = matmul(own_t[s], g[by_src[s]])
        out[at, :] = back + matmul_t(dpre_b[at, :], w_self[...])


def own_work(by_src, own_t, g, dpre_b, w_self):
    own, tb, width = g.shape
    return pl.pallas_call(
        own_kernel,
        out_shape=jax.ShapeDtypeStruct((own * tb, width), F32),
        in_specs=[SMEM] + [VMEM] * 4,
        out_specs=VMEM,
        compiler_params=params(24),
        cost_estimate=cost(1e10, 10 * own * tb * width),
        name="own_work",
    )(by_src, own_t, g, dpre_b, w_self)


def scatter_kernel(
    targets_in, base_in, returned_in, out_in, targets, base, returned, out, stage, sems, *sums
):
    rows, width = base.shape
    peers, slots = targets.shape
    halves = width // LANES
    copies = [
        pltpu.make_async_copy(targets_in, targets, sems.at[0]),
        pltpu.make_async_copy(base_in, base, sems.at[1]),
    ]
    parts = 4
    each = peers // parts
    for c in range(parts):
        at = pl.ds(c * each, each)
        copies.append(pltpu.make_async_copy(returned_in.at[at], returned.at[at], sems.at[3 + c]))
    copies.append(copies.pop(1))
    for copy in copies:
        copy.start()
    for total in sums:
        total[...] = jnp.zeros_like(total)
    copies[0].wait()

    for c in range(parts):
        copies[1 + c].wait()

        @pl.loop(c * each, (c + 1) * each)
        def _(p):
            loosen(stage, 0, returned[p])
            for k in range(0, slots, len(sums)):
                places = [row_at(targets[p, k + j], halves) for j in range(len(sums))]
                values = [
                    total[place, :] + stage[row_at(k + j, halves), :]
                    for j, (total, place) in enumerate(zip(sums, places))
                ]
                for total, place, value in zip(sums, places, values):
                    total[place, :] = value

    copies[1 + parts].wait()
    block = 256

    @pl.loop(0, rows // block)
    def _(i):
        first = pl.multiple_of(i * block, block)
        at = pl.ds(first, block)
        value = base[at, :]
        for total in sums:
            value += tighten(total, first, block, halves)
        out[at, :] = value
        pltpu.make_async_copy(out.at[at], out_in.at[at], sems.at[2]).start()

    pltpu.make_async_copy(out, out_in, sems.at[2]).wait()


def scatter_rows(targets, base, returned):
    rows, width = base.shape
    peers, slots = targets.shape
    halves = width // LANES
    return pl.pallas_call(
        scatter_kernel,
        out_shape=jax.ShapeDtypeStruct((rows, width), F32),
        in_specs=[ANY, ANY, ANY],
        out_specs=ANY,
        scratch_shapes=[
            pltpu.SMEM(targets.shape, jnp.int32),
            pltpu.VMEM((rows, width), F32),
            pltpu.VMEM((peers, slots, width), BF16),
            pltpu.VMEM((rows, width), F32),
            pltpu.VMEM((slots * halves, LANES), F32),
            pltpu.SemaphoreType.DMA((7,)),
        ]
        + [pltpu.VMEM(((rows + 8) * halves, LANES), F32)] * 4,
        compiler_params=params(SCATTER_MIB),
        cost_estimate=cost(1e10, 10 * rows * width),
        name="scatter_rows",
    )(targets, base, returned)


def exchange(block, groups=None):
    return lax.all_to_all(block, AXES, 0, 0, tiled=True, axis_index_groups=groups)


def fetch_rows(features, picks, counts, shape):
    n_row, n_col = shape
    members = n_row * n_col
    far_bit = n_col // 2
    if members > MOST_APART:
        (outgoing,) = gather_rows(
            features, picks, counts, lambda me, j: j, n_col, members, False
        )
        return (), exchange(outgoing)
    half = members // 2
    pairs = half // 2
    soon = pairs // 4

    def gather_far(first, count):
        def whom(me, j):
            return me ^ far_mask(far_bit, 2 * first + j)

        return gather_rows(features, picks, counts, whom, n_col, 2 * count, True)

    def cross(blocks, first):
        return tuple(
            flip(block, far_mask(far_bit, 2 * (first + j)), members)
            for j, block in enumerate(blocks)
        )

    first_blocks = gather_far(0, soon)
    crossed = cross(first_blocks, 0)
    features, _ = lax.optimization_barrier((features, first_blocks[0]))
    outgoing = gather_far(soon, pairs - soon)
    crossed += cross(outgoing[: pairs // 2 - soon], soon)
    crossed += cross(outgoing[pairs // 2 - soon :], pairs // 2)
    features, _ = lax.optimization_barrier((features, outgoing[0]))
    far = crossed + tuple(flip(block, 1, members) for block in crossed)
    (outgoing,) = gather_rows(
        features, picks, counts, lambda me, j: near_peer(me, far_bit, j), n_col, half, False
    )
    groups = [[near_peer(side, far_bit, j) for j in range(half)] for side in (0, far_bit)]
    return far, exchange(outgoing, groups)


def flip(value, bit, members):
    return lax.ppermute(value, AXES, [(i, i ^ bit) for i in range(members)])


def split_bits(shape):
    n_row, n_col = shape
    inner = n_col // 4 if n_col % 4 == 0 else n_col
    near = [1 << i for i in range(inner.bit_length() - 1)]
    near += [n_col << i for i in range(n_row.bit_length() - 1)]
    return near, [inner << i for i in range((n_col // inner).bit_length() - 1)]


def share_of_total(terms, shape):
    members = shape[0] * shape[1]
    near, far = split_bits(shape)
    me = lax.axis_index(AXES)
    for bit in near:
        upper = (me & bit) != 0
        half = terms.shape[0] // 2
        low, high = terms[:half], terms[half:]
        terms = jnp.where(upper, high, low) + flip(jnp.where(upper, low, high), bit, members)
    for bit in far:
        terms = terms + flip(terms, bit, members)
    return terms


def share_groups(shape):
    members = shape[0] * shape[1]
    near, _ = split_bits(shape)

    def place(device):
        return sum(1 << (len(near) - 1 - i) for i, bit in enumerate(near) if device & bit)

    mask = sum(near)
    planes = {}
    for device in range(members):
        planes.setdefault(device & ~mask, []).append(device)
    groups = [sorted(plane, key=place) for _, plane in sorted(planes.items())]
    return groups


def on_device(
    shape, features, send_rows, counts, tile_dst, tile_src, tiles, w_self, w_neigh, bias, cotangent
):
    rows, width = features.shape
    _, slots = send_rows.shape[1:]
    picks = send_rows[0]
    far, near = fetch_rows(features, picks, counts, shape)
    adj, edge_t, own_t, by_src, by_turn, scale = local_work(
        tile_src, tile_dst, tiles[0], rows // slots, shape[1], shape[1] // 2 if far else 0
    )
    keep = jnp.arange(slots, dtype=jnp.int32)[None, :] < counts[0][:, None]
    targets = jnp.where(keep, picks, rows)
    agg, back_b = middle_work(
        far,
        near,
        by_src,
        by_turn,
        adj,
        edge_t,
        features,
        cotangent,
        scale,
        w_self,
        w_neigh,
        bias[None],
    )
    returned = exchange(back_b)
    spare = 8 << len(split_bits(shape)[0])
    layer_out, dpre_b, g, terms = tail_work(
        agg, features, cotangent, scale, w_self, w_neigh, bias[None], spare
    )
    own_grad = own_work(by_src, own_t, g, dpre_b, w_self)
    inv_root = 1.0 / jnp.sqrt(F32(rows * shape[0] * shape[1]))
    share = share_of_total(terms, shape) * inv_root
    groups = share_groups(shape)
    packed = jnp.broadcast_to(share[None], (len(groups[0]),) + share.shape)
    packed, returned = lax.optimization_barrier((packed, returned))
    terms = exchange(packed, groups).reshape(terms.shape)
    grad_features = scatter_rows(targets, own_grad, returned)
    grad_bias = jnp.sum(terms[2 * width : 2 * width + 8], axis=0)
    return layer_out, grad_features, terms[:width], terms[width : 2 * width], grad_bias


def solution(mesh):
    both = P(AXES)
    in_specs = (both,) * 6 + (P(),) * 3 + (both,)
    out_specs = (both, both, P(), P(), P())
    shape = (mesh.shape["row"], mesh.shape["col"])
    return jax.shard_map(
        functools.partial(on_device, shape),
        mesh=mesh,
        in_specs=in_specs,
        out_specs=out_specs,
        check_vma=False,
    )
```
